128 devices in a mesh: row: 16 (over x, z_lo, core), col: 8 (over y, z_hi).
Axes of the slice: x: 4, y: 4, z: 4 (z_hi: 2, z_lo: 2; z = z_hi * 2 + z_lo), core: 2. Of those that a mesh axis runs over, the one named last changes fastest.
Arguments:
- source: float32 [512, 512, 512], P('row', 'col'), may hold values from -8 to 8
- basis_x: float32 [512, 512], replicated, may hold values from -0.25 to 0.25
- basis_y: float32 [512, 512], replicated, may hold values from -0.25 to 0.25
- basis_z: float32 [512, 512], replicated, may hold values from -0.25 to 0.25
- eigen_x: float32 [512], replicated, may hold values from 0.1 to 10
- eigen_y: float32 [512], replicated, may hold values from 0.1 to 10
- eigen_z: float32 [512], replicated, may hold values from 0.1 to 10
Outputs:
- solution: float32 [512, 512, 512], P('row', 'col')
The draws below stay inside these ranges and needn't reach their ends.
All inputs are finite; a program needn't handle non-finite values.
Results may differ from the reference program's by a relative error of at most 0.00007.
Values sent between devices are 32-bit elements; how exact they have to be, the bound alone decides.
No kernel may reach another device: no remote copies, remote signals or barrier semaphores. Data moves between devices by JAX's collectives and lax.ppermute only.
A program may use at most 128 MiB of HBM per device.

```python
import math
import jax
import jax.numpy as jnp
from jax import lax

NX = 512
NY = 512
NZ = 512


def levels(stream_key, extent, cuts, smallest, top_value):
    level, own = 1.0, jax.random.fold_in(stream_key, 6)
    for axis_at, parts in cuts:
        draws = jnp.exp(jax.random.uniform(jax.random.fold_in(own, axis_at), (parts,), jnp.float32, smallest / len(cuts), top_value / len(cuts)))
        level = level * jnp.repeat(draws, extent[axis_at] // parts).reshape([-1 if axis == axis_at else 1 for axis in range(len(extent))])
    return level


def gaussian(stream_key, extent, width, limit, split=(), held_as=jnp.bfloat16):
    values = jax.random.normal(stream_key, extent, jnp.float32) * width
    if len(split) > 0:
        values = levels(stream_key, extent, split, -0.22, 0.18) * values
    return jnp.clip(values, min=-limit, max=limit).astype(held_as)


def setup_inputs(seed: int = 0) -> dict:
    keys = jax.random.split(jax.random.key(seed), 8)
    source = gaussian(keys[0], (NX, NY, NZ), 1.0, 8.0, ((0, 16), (1, 8)), jnp.float32)
    basis_x = gaussian(keys[1], (NX, NX), NX ** -0.5, 0.25, (), jnp.float32)
    basis_y = gaussian(keys[2], (NY, NY), NY ** -0.5, 0.25, (), jnp.float32)
    basis_z = gaussian(keys[3], (NZ, NZ), NZ ** -0.5, 0.25, (), jnp.float32)
    eigen_x = jnp.clip(jnp.exp(jax.random.uniform(keys[4], (NX,), jnp.float32, math.log(0.1), math.log(10.0))), 0.1, 10.0)
    eigen_y = jnp.clip(jnp.exp(jax.random.uniform(keys[5], (NY,), jnp.float32, math.log(0.1), math.log(10.0))), 0.1, 10.0)
    eigen_z = jnp.clip(jnp.exp(jax.random.uniform(keys[6], (NZ,), jnp.float32, math.log(0.1), math.log(10.0))), 0.1, 10.0)
    return {"source": source, "basis_x": basis_x, "basis_y": basis_y, "basis_z": basis_z, "eigen_x": eigen_x, "eigen_y": eigen_y, "eigen_z": eigen_z}


HIGH = lax.Precision.HIGHEST


def reference(source, basis_x, basis_y, basis_z, eigen_x, eigen_y, eigen_z):
    field = jnp.einsum('ai,abc->ibc', basis_x, source, precision=HIGH)
    field = jnp.einsum('bj,ibc->ijc', basis_y, field, precision=HIGH)
    field = jnp.einsum('ck,ijc->ijk', basis_z, field, precision=HIGH)
    denom = eigen_x[:, None, None] + eigen_y[None, :, None] + eigen_z[None, None, :]
    field = field / denom
    field = jnp.einsum('ck,ijk->ijc', basis_z, field, precision=HIGH)
    field = jnp.einsum('bj,ijc->ibc', basis_y, field, precision=HIGH)
    field = jnp.einsum('ai,ibc->abc', basis_x, field, precision=HIGH)
    return field
```

```python
import functools

import jax
import jax.numpy as jnp
from jax import lax
from jax.experimental import pallas as pl
from jax.experimental.pallas import tpu as pltpu
from jax.sharding import PartitionSpec as P

F32 = jnp.float32
BF16 = jnp.bfloat16
AXES = ("row", "col")
NT = (((1,), (1,)), ((), ()))
NN = (((1,), (0,)), ((), ()))


def halves(value):
    high = value.astype(BF16)
    low = (value - high.astype(F32)).astype(BF16)
    return high, low


def product(left, right, dims=NN):
    return lax.dot_general(left, right, dims, preferred_element_type=F32)


def product3(left, right, dims=NN):
    left_high, left_low = left
    right_high, right_low = right
    return (
        product(left_high, right_high, dims)
        + product(left_high, right_low, dims)
        + product(left_low, right_high, dims)
    )


def forward_z(source_ref, basis_ref, out_ref, high_ref, low_ref):
    @pl.when(pl.program_id(0) == 0)
    def _():
        high_ref[...], low_ref[...] = halves(basis_ref[...].T)

    n_z = basis_ref.shape[0]
    flat = out_ref.reshape(n_z * 8, 128)
    for pair in range(4):
        part = halves(source_ref[pl.ds(pair * 256, 256), :])
        result = product3((high_ref[...], low_ref[...]), part, NT)
        flat[pl.ds(2 * pair, n_z, stride=8), :] = result[:, :128]
        flat[pl.ds(2 * pair + 1, n_z, stride=8), :] = result[:, 128:]


def backward_z(field_ref, basis_ref, out_ref, high_ref, low_ref):
    @pl.when(pl.program_id(0) == 0)
    def _():
        high_ref[...], low_ref[...] = halves(basis_ref[...].T)

    n_z = basis_ref.shape[0]
    flat = field_ref.reshape(n_z * 8, 128)
    for pair in range(4):
        lines = jnp.concatenate(
            [flat[pl.ds(2 * pair + side, n_z, stride=8), :].T for side in range(2)], axis=0
        )
        out_ref[pl.ds(pair * 256, 256), :] = product3(
            halves(lines), (high_ref[...], low_ref[...])
        )


def prepare(
    basis_x, basis_y, eigen_x,
    xt_high, xt_low, x_high, x_low, y_high, y_low, yt_high, yt_low, column, strips,
):
    half = basis_x.shape[0] // 2
    for strip in range(strips.shape[0]):
        strips[strip] = basis_x[:, pl.ds(strip * 128, 128)]
    ordered = jnp.concatenate(
        [
            jnp.concatenate(
                [strips[strip, pl.ds(side, half, stride=2), :] for strip in range(strips.shape[0])],
                axis=1,
            )
            for side in range(2)
        ],
        axis=0,
    )
    x_high[...], x_low[...] = halves(ordered)
    xt_high[...], xt_low[...] = halves(ordered.T)
    y_high[...], y_low[...] = halves(basis_y[...])
    yt_high[...], yt_low[...] = halves(basis_y[...].T)
    column[...] = jnp.broadcast_to(eigen_x[...], (128, eigen_x.shape[1])).T


def planes(
    field_ref, xt_high, xt_low, x_high, x_low, y_high, y_low, yt_high, yt_low,
    column, eigen_y, part_z, out_ref, plane_high, plane_low,
):
    rows_n, cols_n = field_ref.shape[0], field_ref.shape[1]
    half = rows_n * 16
    first = lax.broadcasted_iota(jnp.int32, (half, 128), 1) < 64
    for pair in range(cols_n // 2):
        left = field_ref[:, 2 * pair].reshape(half, 128)
        right = field_ref[:, 2 * pair + 1].reshape(half, 128)
        even = jnp.where(first, left, pltpu.roll(right, 64, 1))
        odd = jnp.where(first, pltpu.roll(left, 64, 1), right)
        at = pl.ds(pair * 128, 128)
        plane_high[pl.ds(0, half), at], plane_low[pl.ds(0, half), at] = halves(even)
        plane_high[pl.ds(half, half), at], plane_low[pl.ds(half, half), at] = halves(odd)
    field = product3((xt_high[...], xt_low[...]), (plane_high[...], plane_low[...]))
    field = product3(halves(field), (y_high[...], y_low[...]))
    denom = column[:, :1] + (eigen_y[...] + part_z[pl.program_id(0)])
    field = field / denom
    field = product3(halves(field), (yt_high[...], yt_low[...]))
    field = product3((x_high[...], x_low[...]), halves(field))
    for pair in range(cols_n // 2):
        even = field[:half, pair * 128 : pair * 128 + 128]
        odd = field[half:, pair * 128 : pair * 128 + 128]
        left = jnp.where(first, even, pltpu.roll(odd, 64, 1))
        right = jnp.where(first, pltpu.roll(even, 64, 1), odd)
        out_ref[:, 2 * pair] = left.reshape(rows_n, 2, 1, 8, 128)
        out_ref[:, 2 * pair + 1] = right.reshape(rows_n, 2, 1, 8, 128)


def whole(shape):
    return pl.BlockSpec(shape, lambda step: (0,) * len(shape))


def local(source, basis_x, basis_y, basis_z, eigen_x, eigen_y, eigen_z):
    rows_n, cols_n = lax.axis_size("row"), lax.axis_size("col")
    devices = rows_n * cols_n
    n = basis_z.shape[0]
    square = (n, n)
    lines = source.shape[0] * source.shape[1]
    params = pltpu.CompilerParams(dimension_semantics=("arbitrary",))

    sent = pl.pallas_call(
        forward_z,
        out_shape=jax.ShapeDtypeStruct((devices, 64, 128), F32),
        grid=(2,),
        in_specs=[pl.BlockSpec((lines // 2, n), lambda step: (step, 0)), whole(square)],
        out_specs=pl.BlockSpec((devices, 32, 128), lambda step: (0, step, 0)),
        scratch_shapes=[pltpu.VMEM(square, BF16)] * 2,
        compiler_params=params,
        name="forward_z",
    )(source.reshape(lines, n), basis_z)
    field = lax.all_to_all(sent, AXES, split_axis=0, concat_axis=0, tiled=True)

    tables = pl.pallas_call(
        prepare,
        out_shape=[jax.ShapeDtypeStruct(square, BF16)] * 8 + [jax.ShapeDtypeStruct((n, 128), F32)],
        scratch_shapes=[pltpu.VMEM((n // 128, n, 128), F32)],
        name="prepare",
    )(basis_x, basis_y, eigen_x.reshape(1, n))
    device = lax.axis_index("row") * cols_n + lax.axis_index("col")
    part_z = lax.dynamic_slice_in_dim(eigen_z, device * 4, 4, 0)
    block = pl.BlockSpec((rows_n, cols_n, 2, 1, 8, 128), lambda step: (0, 0, 0, step, 0, 0))
    shape = (rows_n, cols_n, 2, 4, 8, 128)
    field = pl.pallas_call(
        planes,
        out_shape=jax.ShapeDtypeStruct(shape, F32),
        grid=(4,),
        in_specs=[block]
        + [whole(square)] * 8
        + [whole((n, 128)), whole((1, n)), pl.BlockSpec(memory_space=pltpu.SMEM)],
        out_specs=block,
        scratch_shapes=[pltpu.VMEM(square, BF16)] * 2,
        compiler_params=params,
        name="planes",
    )(field.reshape(shape), *tables, eigen_y.reshape(1, n), part_z)

    field = field.reshape(devices, 64, 128)
    field = lax.all_to_all(field, AXES, split_axis=0, concat_axis=0, tiled=True)
    out = pl.pallas_call(
        backward_z,
        out_shape=jax.ShapeDtypeStruct((lines, n), F32),
        grid=(2,),
        in_specs=[pl.BlockSpec((devices, 32, 128), lambda step: (0, step, 0)), whole(square)],
        out_specs=pl.BlockSpec((lines // 2, n), lambda step: (step, 0)),
        scratch_shapes=[pltpu.VMEM(square, BF16)] * 2,
        compiler_params=params,
        name="backward_z",
    )(field, basis_z)
    return out.reshape(source.shape)


def solution(mesh):
    placed = (P("row", "col", None), P(), P(), P(), P(), P(), P())
    return jax.shard_map(
        local, mesh=mesh, in_specs=placed, out_specs=P("row", "col", None), check_vma=False
    )
```

```python
import jax
import jax.numpy as jnp
from jax import lax
from jax.experimental import pallas as pl
from jax.experimental.pallas import tpu as pltpu
from jax.sharding import PartitionSpec as P

F32 = jnp.float32
BF16 = jnp.bfloat16
AXES = ("row", "col")
NT = (((1,), (1,)), ((), ()))
NN = (((1,), (0,)), ((), ()))
MIB = 1 << 20


def halves(value):
    high = value.astype(BF16)
    low = (value - high.astype(F32)).astype(BF16)
    return high, low


def product(left, right, dims=NN):
    return lax.dot_general(left, right, dims, preferred_element_type=F32)


def product3(left, right, dims=NN):
    left_high, left_low = left
    right_high, right_low = right
    return (
        product(left_high, right_high, dims)
        + product(left_high, right_low, dims)
        + product(left_low, right_high, dims)
    )


def forward_z(
    source_hbm, basis_hbm, out_hbm, high_hbm, low_hbm,
    source_ref, basis_ref, out_ref, high_ref, low_ref, sems,
):
    n_z = basis_ref.shape[0]
    parts = source_ref.shape[0] // 512
    reads = [pltpu.make_async_copy(basis_hbm, basis_ref, sems.at[parts])]
    for part in range(parts):
        at = pl.ds(part * 512, 512)
        reads.append(pltpu.make_async_copy(source_hbm.at[at], source_ref.at[at], sems.at[part]))
    for read in reads:
        read.start()
    reads[0].wait()
    high_ref[...], low_ref[...] = halves(basis_ref[...].T)
    writes = [
        pltpu.make_async_copy(high_ref, high_hbm, sems.at[parts + 1]),
        pltpu.make_async_copy(low_ref, low_hbm, sems.at[parts + 2]),
    ]
    for write in writes:
        write.start()
    flat = out_ref.reshape(n_z * 16, 128)
    for pair in range(2 * parts):
        if pair % 2 == 0:
            reads[1 + pair // 2].wait()
        lines = halves(source_ref[pl.ds(pair * 256, 256), :])
        result = product3((high_ref[...], low_ref[...]), lines, NT)
        flat[pl.ds(2 * pair, n_z, stride=16), :] = result[:, :128]
        flat[pl.ds(2 * pair + 1, n_z, stride=16), :] = result[:, 128:]
        if pair % 4 == 3:
            at = pl.ds(pair // 4 * 8, 8)
            writes.append(
                pltpu.make_async_copy(
                    out_ref.at[:, :, at], out_hbm.at[:, :, at], sems.at[parts + 3 + pair // 4]
                )
            )
            writes[-1].start()
    for write in writes:
        write.wait()


def backward_z(field_ref, high_ref, low_ref, out_hbm, out_ref, sems):
    n_z = high_ref.shape[0]
    flat = field_ref.reshape(n_z * 16, 128)
    copies = []
    for part in range(out_ref.shape[0] // 512):
        for pair in range(2):
            first = part * 4 + pair * 2
            lines = jnp.concatenate(
                [flat[pl.ds(first + side, n_z, stride=16), :].T for side in range(2)], axis=0
            )
            out_ref[pl.ds(first * 128, 256), :] = product3(
                halves(lines), (high_ref[...], low_ref[...])
            )
        at = pl.ds(part * 512, 512)
        copies.append(pltpu.make_async_copy(out_ref.at[at], out_hbm.at[at], sems.at[part]))
        copies[-1].start()
    for copy in copies:
        copy.wait()


def prepare(
    basis_x, basis_y, eigen_x,
    xt_high, xt_low, x_high, x_low, y_high, y_low, yt_high, yt_low, column, strips,
):
    half = basis_x.shape[0] // 2
    for strip in range(strips.shape[0]):
        strips[strip] = basis_x[:, pl.ds(strip * 128, 128)]
    ordered = jnp.concatenate(
        [
            jnp.concatenate(
                [strips[strip, pl.ds(side, half, stride=2), :] for strip in range(strips.shape[0])],
                axis=1,
            )
            for side in range(2)
        ],
        axis=0,
    )
    x_high[...], x_low[...] = halves(ordered)
    xt_high[...], xt_low[...] = halves(ordered.T)
    y_high[...], y_low[...] = halves(basis_y[...])
    yt_high[...], yt_low[...] = halves(basis_y[...].T)
    column[...] = jnp.broadcast_to(eigen_x[...], (128, eigen_x.shape[1])).T


def planes(
    field_hbm, xt_high_hbm, xt_low_hbm, x_high_hbm, x_low_hbm,
    y_high_hbm, y_low_hbm, yt_high_hbm, yt_low_hbm, column_hbm, eigen_y, part_z, out_ref,
    field_ref, xt_high, xt_low, x_high, x_low, y_high, y_low, yt_high, yt_low, column,
    plane_high, plane_low, sems,
):
    count, rows_n, cols_n = field_ref.shape[:3]
    half = rows_n * 16
    first = lax.broadcasted_iota(jnp.int32, (half, 128), 1) < 64

    def read_plane(plane):
        return pltpu.make_async_copy(field_hbm.at[:, :, plane], field_ref.at[plane], sems.at[plane])

    tables = [
        pltpu.make_async_copy(source, target, sems.at[count + at])
        for at, (source, target) in enumerate(
            (
                (xt_high_hbm, xt_high), (xt_low_hbm, xt_low), (y_high_hbm, y_high),
                (y_low_hbm, y_low), (column_hbm, column), (yt_high_hbm, yt_high),
                (yt_low_hbm, yt_low), (x_high_hbm, x_high), (x_low_hbm, x_low),
            )
        )
    ]
    read_plane(0).start()
    tables[0].start()
    tables[1].start()
    read_plane(1).start()
    for table in tables[2:]:
        table.start()
    for plane in range(2, count):
        read_plane(plane).start()

    def gather(plane, side):
        read_plane(plane).wait()
        for pair in range(cols_n // 2):
            left = field_ref[plane, :, 2 * pair].reshape(half, 128)
            right = field_ref[plane, :, 2 * pair + 1].reshape(half, 128)
            even = jnp.where(first, left, pltpu.roll(right, 64, 1))
            odd = jnp.where(first, pltpu.roll(left, 64, 1), right)
            at = pl.ds(pair * 128, 128)
            for rows, value in ((pl.ds(0, half), even), (pl.ds(half, half), odd)):
                plane_high[side, rows, at], plane_low[side, rows, at] = halves(value)

    def scatter(plane, field):
        for pair in range(cols_n // 2):
            even = field[:half, pair * 128 : pair * 128 + 128]
            odd = field[half:, pair * 128 : pair * 128 + 128]
            left = jnp.where(first, even, pltpu.roll(odd, 64, 1))
            right = jnp.where(first, pltpu.roll(even, 64, 1), odd)
            out_ref[:, 2 * pair, plane] = left.reshape(rows_n, 16, 128)
            out_ref[:, 2 * pair + 1, plane] = right.reshape(rows_n, 16, 128)

    tables[0].wait()
    tables[1].wait()

    @pl.loop(0, count // 2)
    def _(step):
        sides = range(2)
        fields = [None, None]
        gather(2 * step, 0)
        for side in sides:
            if side == 0:
                gather(2 * step + 1, 1)
            fields[side] = product3(
                (xt_high[...], xt_low[...]), (plane_high[side], plane_low[side])
            )

        @pl.when(step == 0)
        def _():
            for table in tables[2:]:
                table.wait()

        for side in sides:
            fields[side] = product3(halves(fields[side]), (y_high[...], y_low[...]))
        for side in sides:
            denom = column[:, :1] + (eigen_y[...] + part_z[2 * step + side])
            fields[side] = product3(halves(fields[side] / denom), (yt_high[...], yt_low[...]))
        for side in sides:
            fields[side] = product3((x_high[...], x_low[...]), halves(fields[side]))
            scatter(2 * step + side, fields[side])


VMEM_SPEC = pl.BlockSpec(memory_space=pltpu.VMEM)
HBM_SPEC = pl.BlockSpec(memory_space=pltpu.HBM)


def limit(mebibytes):
    return pltpu.CompilerParams(vmem_limit_bytes=mebibytes * MIB)


def local(source, basis_x, basis_y, basis_z, eigen_x, eigen_y, eigen_z):
    rows_n, cols_n = lax.axis_size("row"), lax.axis_size("col")
    devices = rows_n * cols_n
    n = basis_z.shape[0]
    square = (n, n)
    lines = source.shape[0] * source.shape[1]
    table = jax.ShapeDtypeStruct(square, BF16)

    sent, z_high, z_low = pl.pallas_call(
        forward_z,
        out_shape=[jax.ShapeDtypeStruct((devices, 4, 16, 128), F32), table, table],
        in_specs=[HBM_SPEC] * 2,
        out_specs=[HBM_SPEC] * 3,
        scratch_shapes=[
            pltpu.VMEM((lines, n), F32),
            pltpu.VMEM(square, F32),
            pltpu.VMEM((devices, 4, 16, 128), F32),
            pltpu.VMEM(square, BF16),
            pltpu.VMEM(square, BF16),
            pltpu.SemaphoreType.DMA((lines // 512 + 5,)),
        ],
        name="forward_z",
    )(source.reshape(lines, n), basis_z)
    sent = sent.reshape(devices, 64, 128)
    field = lax.all_to_all(sent, AXES, split_axis=0, concat_axis=0, tiled=True)

    tables = pl.pallas_call(
        prepare,
        out_shape=[table] * 8 + [jax.ShapeDtypeStruct((n, 128), F32)],
        scratch_shapes=[pltpu.VMEM((n // 128, n, 128), F32)],
        name="prepare",
    )(basis_x, basis_y, eigen_x.reshape(1, n))
    device = lax.axis_index("row") * cols_n + lax.axis_index("col")
    part_z = lax.dynamic_slice_in_dim(eigen_z, device * 4, 4, 0)
    shape = (rows_n, cols_n, 4, 16, 128)
    field = pl.pallas_call(
        planes,
        out_shape=jax.ShapeDtypeStruct(shape, F32),
        in_specs=[HBM_SPEC] * 10 + [VMEM_SPEC, pl.BlockSpec(memory_space=pltpu.SMEM)],
        out_specs=VMEM_SPEC,
        scratch_shapes=[pltpu.VMEM((4, rows_n, cols_n, 16, 128), F32)]
        + [pltpu.VMEM(square, BF16)] * 8
        + [pltpu.VMEM((n, 128), F32)]
        + [pltpu.VMEM((2,) + square, BF16)] * 2
        + [pltpu.SemaphoreType.DMA((13,))],
        compiler_params=limit(40),
        name="planes",
    )(*[pltpu.with_memory_space_constraint(a, pltpu.HBM) for a in (field.reshape(shape), *tables)], eigen_y.reshape(1, n), part_z)

    field = field.reshape(devices, 64, 128)
    field = lax.all_to_all(field, AXES, split_axis=0, concat_axis=0, tiled=True)
    out = pl.pallas_call(
        backward_z,
        out_shape=jax.ShapeDtypeStruct((lines, n), F32),
        in_specs=[VMEM_SPEC] * 3,
        out_specs=HBM_SPEC,
        scratch_shapes=[
            pltpu.VMEM((lines, n), F32), pltpu.SemaphoreType.DMA((lines // 512,))
        ],
        compiler_params=limit(20),
        name="backward_z",
    )(field, z_high, z_low)
    return out.reshape(source.shape)


def solution(mesh):
    placed = (P("row", "col", None), P(), P(), P(), P(), P(), P())
    return jax.shard_map(
        local, mesh=mesh, in_specs=placed, out_specs=P("row", "col", None), check_vma=False
    )
```

```python
import jax
import jax.numpy as jnp
from jax import lax
from jax.experimental import pallas as pl
from jax.experimental.pallas import tpu as pltpu
from jax.sharding import PartitionSpec as P

F32 = jnp.float32
BF16 = jnp.bfloat16
AXES = ("row", "col")
NT = (((1,), (1,)), ((), ()))
NN = (((1,), (0,)), ((), ()))
MIB = 1 << 20


def halves(value):
    high = value.astype(BF16)
    low = (value - high.astype(F32)).astype(BF16)
    return high, low


def product(left, right, dims=NN):
    return lax.dot_general(left, right, dims, preferred_element_type=F32)


def product3(left, right, dims=NN):
    left_high, left_low = left
    right_high, right_low = right
    return (
        product(left_high, right_high, dims)
        + product(left_high, right_low, dims)
        + product(left_low, right_high, dims)
    )


def forward_z(
    source_hbm, basis_hbm, out_hbm, both_hbm, source_ref, basis_ref, out_ref, both_ref, sems,
):
    n_z = basis_ref.shape[0]
    parts = source_ref.shape[0] // 512
    reads = [pltpu.make_async_copy(basis_hbm, basis_ref, sems.at[parts])]
    for part in range(parts):
        at = pl.ds(part * 512, 512)
        reads.append(pltpu.make_async_copy(source_hbm.at[at], source_ref.at[at], sems.at[part]))
    for read in reads:
        read.start()
    reads[0].wait()
    both_ref[pl.ds(0, n_z), :], both_ref[pl.ds(n_z, n_z), :] = halves(basis_ref[...].T)
    writes = [pltpu.make_async_copy(both_ref, both_hbm, sems.at[parts + 1])]
    writes[0].start()
    flat = out_ref.reshape(2 * n_z * 8, 128)
    for pair in range(2 * parts):
        if pair % 4 == 0:
            reads[1 + pair // 2].wait()
            reads[2 + pair // 2].wait()
        high, low = halves(source_ref[pl.ds(pair * 256, 256), :])
        result = product(both_ref[...], high, NT)
        result = result[:n_z] + result[n_z:] + product(both_ref[pl.ds(0, n_z), :], low, NT)
        half = pair // 4
        for side in range(2):
            at = half * n_z * 8 + pair % 4 * 2 + side
            flat[pl.ds(at, n_z, stride=8), :] = result[:, side * 128 : side * 128 + 128]
        if pair % 4 == 3:
            writes.append(
                pltpu.make_async_copy(
                    out_ref.at[half], out_hbm.at[:, half], sems.at[parts + 2 + half]
                )
            )
            writes[-1].start()
    for write in writes:
        write.wait()


def backward_z(field_ref, both_ref, out_hbm, tiles_ref, out_ref, sems):
    n_z = both_ref.shape[0] // 2
    table = both_ref[pl.ds(0, n_z), :], both_ref[pl.ds(n_z, n_z), :]
    writes = []
    for half in range(2):
        tiles_ref[half] = field_ref[:, :, pl.ds(half * 8, 8), :].reshape(n_z * 8, 128)
        for pair in range(4):
            lines = jnp.concatenate(
                [
                    tiles_ref[half, pl.ds(pair * 2 + side, n_z, stride=8), :].T
                    for side in range(2)
                ],
                axis=0,
            )
            at = pl.ds((half * 4 + pair) * 256, 256)
            out_ref[at, :] = product3(halves(lines), table)
            writes.append(
                pltpu.make_async_copy(out_ref.at[at], out_hbm.at[at], sems.at[half * 4 + pair])
            )
            writes[-1].start()
    for write in writes:
        write.wait()


def prepare(
    basis_x, basis_y, eigen_x,
    xt_high, xt_low, x_high, x_low, y_high, y_low, yt_high, yt_low, column, strips,
):
    half = basis_x.shape[0] // 2
    for strip in range(strips.shape[0]):
        strips[strip] = basis_x[:, pl.ds(strip * 128, 128)]
    ordered = jnp.concatenate(
        [
            jnp.concatenate(
                [strips[strip, pl.ds(side, half, stride=2), :] for strip in range(strips.shape[0])],
                axis=1,
            )
            for side in range(2)
        ],
        axis=0,
    )
    x_high[...], x_low[...] = halves(ordered)
    xt_high[...], xt_low[...] = halves(ordered.T)
    y_high[...], y_low[...] = halves(basis_y[...])
    yt_high[...], yt_low[...] = halves(basis_y[...].T)
    column[...] = jnp.broadcast_to(eigen_x[...], (128, eigen_x.shape[1])).T


def planes(
    field_hbm, xt_high_hbm, xt_low_hbm, x_high_hbm, x_low_hbm,
    y_high_hbm, y_low_hbm, yt_high_hbm, yt_low_hbm, column_hbm, eigen_y, eigen_z, out_ref,
    field_ref, xt_high, xt_low, x_high, x_low, y_high, y_low, yt_high, yt_low, column,
    plane_high, plane_low, sems,
):
    count, rows_n, cols_n = field_ref.shape[:3]
    owned = (lax.axis_index("row") * cols_n + lax.axis_index("col")) * count
    half = rows_n * 16
    lower = lax.broadcasted_iota(jnp.int32, (half, 128), 1) < 64

    def read_plane(plane):
        return pltpu.make_async_copy(field_hbm.at[:, :, :, plane], field_ref.at[plane], sems.at[plane])

    tables = [
        pltpu.make_async_copy(source, target, sems.at[count + at])
        for at, (source, target) in enumerate(
            (
                (xt_high_hbm, xt_high), (xt_low_hbm, xt_low), (y_high_hbm, y_high),
                (y_low_hbm, y_low), (column_hbm, column), (yt_high_hbm, yt_high),
                (yt_low_hbm, yt_low), (x_high_hbm, x_high), (x_low_hbm, x_low),
            )
        )
    ]
    read_plane(0).start()
    tables[0].start()
    tables[1].start()
    read_plane(1).start()
    for table in tables[2:]:
        table.start()
    for plane in range(2, count):
        read_plane(plane).start()

    def gather(plane, side):
        for pair in range(cols_n // 2):
            left = field_ref[plane, :, 2 * pair].reshape(half, 128)
            right = field_ref[plane, :, 2 * pair + 1].reshape(half, 128)
            even = jnp.where(lower, left, pltpu.roll(right, 64, 1))
            odd = jnp.where(lower, pltpu.roll(left, 64, 1), right)
            at = pl.ds(pair * 128, 128)
            for rows, value in ((pl.ds(0, half), even), (pl.ds(half, half), odd)):
                plane_high[side, rows, at], plane_low[side, rows, at] = halves(value)

    def scatter(plane, field):
        for pair in range(cols_n // 2):
            even = field[:half, pair * 128 : pair * 128 + 128]
            odd = field[half:, pair * 128 : pair * 128 + 128]
            left = jnp.where(lower, even, pltpu.roll(odd, 64, 1))
            right = jnp.where(lower, pltpu.roll(even, 64, 1), odd)
            out_ref[:, 2 * pair, plane] = left.reshape(rows_n, 16, 128)
            out_ref[:, 2 * pair + 1, plane] = right.reshape(rows_n, 16, 128)

    fields = [None] * count

    def into_x(plane):
        side = plane % 2
        fields[plane] = product3(
            (xt_high[...], xt_low[...]), (plane_high[side], plane_low[side])
        )

    def into_y(plane):
        fields[plane] = product3(halves(fields[plane]), (y_high[...], y_low[...]))

    def out_of_y(plane):
        denom = column[:, :1] + (eigen_y[...] + eigen_z[owned + plane])
        fields[plane] = product3(halves(fields[plane] / denom), (yt_high[...], yt_low[...]))

    def out_of_x(plane):
        fields[plane] = product3((x_high[...], x_low[...]), halves(fields[plane]))

    read_plane(0).wait()
    gather(0, 0)
    read_plane(1).wait()
    tables[0].wait()
    tables[1].wait()
    for first in range(0, count, 2):
        second = first + 1
        into_x(first)
        gather(second, 1)
        if first > 0:
            scatter(first - 1, fields[first - 1])
        into_x(second)
        if first == 0:
            for table in tables[2:]:
                table.wait()
            for plane in range(2, count):
                read_plane(plane).wait()
        for stage in (into_y, out_of_y):
            stage(first)
            stage(second)
        out_of_x(first)
        if second + 1 < count:
            gather(second + 1, 0)
        scatter(first, fields[first])
        out_of_x(second)
    scatter(count - 1, fields[count - 1])


VMEM_SPEC = pl.BlockSpec(memory_space=pltpu.VMEM)
HBM_SPEC = pl.BlockSpec(memory_space=pltpu.HBM)


def limit(mebibytes):
    return pltpu.CompilerParams(vmem_limit_bytes=mebibytes * MIB)


def local(source, basis_x, basis_y, basis_z, eigen_x, eigen_y, eigen_z):
    rows_n, cols_n = lax.axis_size("row"), lax.axis_size("col")
    devices = rows_n * cols_n
    n = basis_z.shape[0]
    square = (n, n)
    lines = source.shape[0] * source.shape[1]
    table = jax.ShapeDtypeStruct(square, BF16)

    both = jax.ShapeDtypeStruct((2 * n, n), BF16)
    sent, both_z = pl.pallas_call(
        forward_z,
        out_shape=[jax.ShapeDtypeStruct((devices, 2, 32, 128), F32), both],
        in_specs=[HBM_SPEC] * 2,
        out_specs=[HBM_SPEC] * 2,
        scratch_shapes=[
            pltpu.VMEM((lines, n), F32),
            pltpu.VMEM(square, F32),
            pltpu.VMEM((2, devices, 32, 128), F32),
            pltpu.VMEM((2 * n, n), BF16),
            pltpu.SemaphoreType.DMA((lines // 512 + 4,)),
        ],
        name="forward_z",
    )(source.reshape(lines, n), basis_z)
    sent = sent.reshape(devices, 64, 128)
    field = lax.all_to_all(sent, AXES, split_axis=0, concat_axis=0, tiled=True)

    tables = pl.pallas_call(
        prepare,
        out_shape=[table] * 8 + [jax.ShapeDtypeStruct((n, 128), F32)],
        scratch_shapes=[pltpu.VMEM((n // 128, n, 128), F32)],
        name="prepare",
    )(basis_x, basis_y, eigen_x.reshape(1, n))
    shape = (rows_n, cols_n, 4, 16, 128)
    arrived = field.reshape(rows_n, cols_n, 2, 4, 8, 128)
    field = pl.pallas_call(
        planes,
        out_shape=jax.ShapeDtypeStruct(shape, F32),
        in_specs=[HBM_SPEC] * 10 + [VMEM_SPEC, pl.BlockSpec(memory_space=pltpu.SMEM)],
        out_specs=VMEM_SPEC,
        scratch_shapes=[pltpu.VMEM((4, rows_n, cols_n, 2, 8, 128), F32)]
        + [pltpu.VMEM(square, BF16)] * 8
        + [pltpu.VMEM((n, 128), F32)]
        + [pltpu.VMEM((2,) + square, BF16)] * 2
        + [pltpu.SemaphoreType.DMA((13,))],
        compiler_params=limit(40),
        name="planes",
    )(*[pltpu.with_memory_space_constraint(a, pltpu.HBM) for a in (arrived, *tables)], eigen_y.reshape(1, n), eigen_z)

    field = field.reshape(devices, 64, 128)
    field = lax.all_to_all(field, AXES, split_axis=0, concat_axis=0, tiled=True)
    out = pl.pallas_call(
        backward_z,
        out_shape=jax.ShapeDtypeStruct((lines, n), F32),
        in_specs=[VMEM_SPEC] * 2,
        out_specs=HBM_SPEC,
        scratch_shapes=[
            pltpu.VMEM((2, lines * 2, 128), F32),
            pltpu.VMEM((lines, n), F32),
            pltpu.SemaphoreType.DMA((lines // 256,)),
        ],
        compiler_params=limit(20),
        name="backward_z",
    )(field.reshape(devices, 4, 16, 128), both_z)
    return out.reshape(source.shape)


def solution(mesh):
    placed = (P("row", "col", None), P(), P(), P(), P(), P(), P())
    return jax.shard_map(
        local, mesh=mesh, in_specs=placed, out_specs=P("row", "col", None), check_vma=False
    )
```

```python
import jax
import jax.numpy as jnp
from jax import lax
from jax.experimental import pallas as pl
from jax.experimental.pallas import tpu as pltpu
from jax.sharding import PartitionSpec as P

F32 = jnp.float32
BF16 = jnp.bfloat16
AXES = ("row", "col")
NT = (((1,), (1,)), ((), ()))
NN = (((1,), (0,)), ((), ()))
MIB = 1 << 20


def halves(value):
    high = value.astype(BF16)
    low = (value - high.astype(F32)).astype(BF16)
    return high, low


def product(left, right, dims=NN):
    return lax.dot_general(left, right, dims, preferred_element_type=F32)


def product3(left, right, dims=NN):
    left_high, left_low = left
    right_high, right_low = right
    return (
        product(left_high, right_high, dims)
        + product(left_high, right_low, dims)
        + product(left_low, right_high, dims)
    )


def forward_z(source_hbm, basis_hbm, out_ref, both_ref, source_ref, basis_ref, tiles_ref, sems):
    n_z = basis_ref.shape[0]
    parts = source_ref.shape[0] // 512
    reads = [pltpu.make_async_copy(basis_hbm, basis_ref, sems.at[parts])]
    for part in range(parts):
        at = pl.ds(part * 512, 512)
        reads.append(pltpu.make_async_copy(source_hbm.at[at], source_ref.at[at], sems.at[part]))
    for read in reads:
        read.start()
    reads[0].wait()
    both_ref[pl.ds(0, n_z), :], both_ref[pl.ds(n_z, n_z), :] = halves(basis_ref[...].T)
    for pair in range(2 * parts):
        if pair % 4 == 0:
            reads[1 + pair // 2].wait()
            reads[2 + pair // 2].wait()
        high, low = halves(source_ref[pl.ds(pair * 256, 256), :])
        result = product(both_ref[...], high, NT)
        result = result[:n_z] + result[n_z:] + product(both_ref[pl.ds(0, n_z), :], low, NT)
        half = pair // 4
        for side in range(2):
            at = pl.ds(pair % 4 * 2 + side, n_z, stride=8)
            tiles_ref[half, at, :] = result[:, side * 128 : side * 128 + 128]
        if pair % 4 == 3:
            out_ref[:, half] = tiles_ref[half].reshape(out_ref.shape[0], 32, 128)


def backward_z(field_ref, both_ref, out_hbm, tiles_ref, out_ref, sems):
    n_z = both_ref.shape[0] // 2
    table = both_ref[pl.ds(0, n_z), :], both_ref[pl.ds(n_z, n_z), :]
    writes = []
    for half in range(2):
        tiles_ref[half] = field_ref[:, :, pl.ds(half * 8, 8), :].reshape(n_z * 8, 128)
        for pair in range(4):
            lines = jnp.concatenate(
                [
                    tiles_ref[half, pl.ds(pair * 2 + side, n_z, stride=8), :].T
                    for side in range(2)
                ],
                axis=0,
            )
            at = pl.ds((half * 4 + pair) * 256, 256)
            out_ref[at, :] = product3(halves(lines), table)
            writes.append(
                pltpu.make_async_copy(out_ref.at[at], out_hbm.at[at], sems.at[half * 4 + pair])
            )
            writes[-1].start()
    for write in writes:
        write.wait()


def planes(
    field_ref, basis_x, basis_y, eigen_x, eigen_y, eigen_z, out_ref,
    strips, xt_high, xt_low, x_high, x_low, y_high, y_low, yt_high, yt_low, column,
    plane_high, plane_low,
):
    rows_n, cols_n, _, count = field_ref.shape[:4]
    n = basis_x.shape[0]
    half = rows_n * 16
    owned = (lax.axis_index("row") * cols_n + lax.axis_index("col")) * count
    lower = lax.broadcasted_iota(jnp.int32, (half, 128), 1) < 64

    def ordered(strip):
        return jnp.concatenate(
            [strips[strip, pl.ds(side, n // 2, stride=2), :] for side in range(2)], axis=0
        )

    def tables_xt():
        for strip in range(n // 128):
            at = pl.ds(strip * 128, 128)
            strips[strip] = basis_x[:, at]
            xt_high[at, :], xt_low[at, :] = halves(ordered(strip).T)

    def tables_x():
        for strip in range(n // 128):
            at = pl.ds(strip * 128, 128)
            x_high[:, at], x_low[:, at] = halves(ordered(strip))

    def tables_y():
        y_high[...], y_low[...] = halves(basis_y[...])
        column[...] = jnp.broadcast_to(eigen_x[...], (128, n)).T

    def tables_yt():
        yt_high[...], yt_low[...] = halves(basis_y[...].T)

    def gather(plane, side):
        for pair in range(cols_n // 2):
            left = field_ref[:, 2 * pair, :, plane].reshape(half, 128)
            right = field_ref[:, 2 * pair + 1, :, plane].reshape(half, 128)
            even = jnp.where(lower, left, pltpu.roll(right, 64, 1))
            odd = jnp.where(lower, pltpu.roll(left, 64, 1), right)
            at = pl.ds(pair * 128, 128)
            for rows, value in ((pl.ds(0, half), even), (pl.ds(half, half), odd)):
                plane_high[side, rows, at], plane_low[side, rows, at] = halves(value)

    def scatter(plane, field):
        for pair in range(cols_n // 2):
            even = field[:half, pair * 128 : pair * 128 + 128]
            odd = field[half:, pair * 128 : pair * 128 + 128]
            left = jnp.where(lower, even, pltpu.roll(odd, 64, 1))
            right = jnp.where(lower, pltpu.roll(even, 64, 1), odd)
            out_ref[:, 2 * pair, plane] = left.reshape(rows_n, 16, 128)
            out_ref[:, 2 * pair + 1, plane] = right.reshape(rows_n, 16, 128)

    fields = [None] * count

    def into_x(plane):
        side = plane % 2
        fields[plane] = product3(
            (xt_high[...], xt_low[...]), (plane_high[side], plane_low[side])
        )

    def into_y(plane):
        fields[plane] = product3(halves(fields[plane]), (y_high[...], y_low[...]))

    def out_of_y(plane):
        denom = column[:, :1] + (eigen_y[...] + eigen_z[owned + plane])
        fields[plane] = product3(halves(fields[plane] / denom), (yt_high[...], yt_low[...]))

    def out_of_x(plane):
        fields[plane] = product3((x_high[...], x_low[...]), halves(fields[plane]))

    tables_xt()
    gather(0, 0)
    for first in range(0, count, 2):
        second = first + 1
        into_x(first)
        gather(second, 1)
        if first == 0:
            tables_y()
        else:
            scatter(first - 1, fields[first - 1])
        into_x(second)
        if first == 0:
            tables_yt()
            tables_x()
        for stage in (into_y, out_of_y):
            stage(first)
            stage(second)
        out_of_x(first)
        if second + 1 < count:
            gather(second + 1, 0)
        scatter(first, fields[first])
        out_of_x(second)
    scatter(count - 1, fields[count - 1])


VMEM_SPEC = pl.BlockSpec(memory_space=pltpu.VMEM)
HBM_SPEC = pl.BlockSpec(memory_space=pltpu.HBM)


def in_hbm(value):
    return pltpu.with_memory_space_constraint(value, pltpu.HBM)


def limit(mebibytes):
    return pltpu.CompilerParams(vmem_limit_bytes=mebibytes * MIB)


def local(source, basis_x, basis_y, basis_z, eigen_x, eigen_y, eigen_z):
    rows_n, cols_n = lax.axis_size("row"), lax.axis_size("col")
    devices = rows_n * cols_n
    n = basis_z.shape[0]
    square = (n, n)
    lines = source.shape[0] * source.shape[1]

    sent, both_z = pl.pallas_call(
        forward_z,
        out_shape=[
            jax.ShapeDtypeStruct((devices, 2, 32, 128), F32),
            jax.ShapeDtypeStruct((2 * n, n), BF16),
        ],
        in_specs=[HBM_SPEC] * 2,
        out_specs=[VMEM_SPEC] * 2,
        scratch_shapes=[
            pltpu.VMEM((lines, n), F32),
            pltpu.VMEM(square, F32),
            pltpu.VMEM((2, lines * 2, 128), F32),
            pltpu.SemaphoreType.DMA((lines // 512 + 1,)),
        ],
        compiler_params=limit(20),
        name="forward_z",
    )(in_hbm(source.reshape(lines, n)), in_hbm(basis_z))
    sent = sent.reshape(devices, 64, 128)
    field = lax.all_to_all(sent, AXES, split_axis=0, concat_axis=0, tiled=True)

    shape = (rows_n, cols_n, 4, 16, 128)
    field = pl.pallas_call(
        planes,
        out_shape=jax.ShapeDtypeStruct(shape, F32),
        in_specs=[VMEM_SPEC] * 5 + [pl.BlockSpec(memory_space=pltpu.SMEM)],
        out_specs=VMEM_SPEC,
        scratch_shapes=[pltpu.VMEM((n // 128, n, 128), F32)]
        + [pltpu.VMEM(square, BF16)] * 8
        + [pltpu.VMEM((n, 128), F32)]
        + [pltpu.VMEM((2,) + square, BF16)] * 2,
        compiler_params=limit(24),
        name="planes",
    )(
        field.reshape(rows_n, cols_n, 2, 4, 8, 128), basis_x, basis_y,
        eigen_x.reshape(1, n), eigen_y.reshape(1, n), eigen_z,
    )

    field = field.reshape(devices, 64, 128)
    field = lax.all_to_all(field, AXES, split_axis=0, concat_axis=0, tiled=True)
    out = pl.pallas_call(
        backward_z,
        out_shape=jax.ShapeDtypeStruct((lines, n), F32),
        in_specs=[VMEM_SPEC] * 2,
        out_specs=HBM_SPEC,
        scratch_shapes=[
            pltpu.VMEM((2, lines * 2, 128), F32),
            pltpu.VMEM((lines, n), F32),
            pltpu.SemaphoreType.DMA((lines // 256,)),
        ],
        compiler_params=limit(20),
        name="backward_z",
    )(field.reshape(devices, 4, 16, 128), both_z)
    return out.reshape(source.shape)


def solution(mesh):
    placed = (P("row", "col", None), P(), P(), P(), P(), P(), P())
    return jax.shard_map(
        local, mesh=mesh, in_specs=placed, out_specs=P("row", "col", None), check_vma=False
    )
```

```python
import jax
import jax.numpy as jnp
from jax import lax
from jax.experimental import pallas as pl
from jax.experimental.pallas import tpu as pltpu
from jax.sharding import PartitionSpec as P

F32 = jnp.float32
BF16 = jnp.bfloat16
AXES = ("row", "col")
NT = (((1,), (1,)), ((), ()))
NN = (((1,), (0,)), ((), ()))
MIB = 1 << 20


def halves(value):
    high = value.astype(BF16)
    low = (value - high.astype(F32)).astype(BF16)
    return high, low


def product(left, right, dims=NN):
    return lax.dot_general(left, right, dims, preferred_element_type=F32)


def product3(left, right, dims=NN):
    left_high, left_low = left
    right_high, right_low = right
    return (
        product(left_high, right_high, dims)
        + product(left_high, right_low, dims)
        + product(left_low, right_high, dims)
    )


def forward_z(source_hbm, basis_hbm, out_ref, both_ref, source_ref, basis_ref, tiles_ref, sems):
    n_z = basis_ref.shape[0]
    parts = source_ref.shape[0] // 512
    reads = [pltpu.make_async_copy(basis_hbm, basis_ref, sems.at[parts])]
    for part in range(parts):
        at = pl.ds(part * 512, 512)
        reads.append(pltpu.make_async_copy(source_hbm.at[at], source_ref.at[at], sems.at[part]))
    for read in reads:
        read.start()
    reads[0].wait()
    both_ref[pl.ds(0, n_z), :], both_ref[pl.ds(n_z, n_z), :] = halves(basis_ref[...].T)
    for pair in range(2 * parts):
        if pair % 4 == 0:
            reads[1 + pair // 2].wait()
            reads[2 + pair // 2].wait()
        high, low = halves(source_ref[pl.ds(pair * 256, 256), :])
        result = product(both_ref[...], high, NT)
        result = result[:n_z] + result[n_z:] + product(both_ref[pl.ds(0, n_z), :], low, NT)
        half = pair // 4
        for side in range(2):
            at = pl.ds(pair % 4 * 2 + side, n_z, stride=8)
            tiles_ref[half, at, :] = result[:, side * 128 : side * 128 + 128]
        if pair % 4 == 3:
            out_ref[:, half] = tiles_ref[half].reshape(out_ref.shape[0], 32, 128)


def backward_z(field_ref, both_ref, out_hbm, tiles_ref, out_ref, sems):
    n_z = both_ref.shape[0] // 2
    table = both_ref[pl.ds(0, n_z), :], both_ref[pl.ds(n_z, n_z), :]
    writes = []
    for half in range(2):
        tiles_ref[half] = field_ref[:, :, pl.ds(half * 8, 8), :].reshape(n_z * 8, 128)
        for pair in range(4):
            lines = jnp.concatenate(
                [
                    tiles_ref[half, pl.ds(pair * 2 + side, n_z, stride=8), :].T
                    for side in range(2)
                ],
                axis=0,
            )
            at = pl.ds((half * 4 + pair) * 256, 256)
            out_ref[at, :] = product3(halves(lines), table)
            writes.append(
                pltpu.make_async_copy(out_ref.at[at], out_hbm.at[at], sems.at[half * 4 + pair])
            )
            writes[-1].start()
    for write in writes:
        write.wait()


def planes(
    field_ref, basis_x, basis_y, eigen_x, eigen_y, eigen_z, out_ref,
    strips, xt_high, xt_low, x_high, x_low, y_high, y_low, yt_high, yt_low, column,
    plane_high, plane_low,
):
    rows_n, cols_n, _, count = field_ref.shape[:4]
    n = basis_x.shape[0]
    half = rows_n * 16
    owned = (lax.axis_index("row") * cols_n + lax.axis_index("col")) * count
    lower = lax.broadcasted_iota(jnp.int32, (half, 128), 1) < 64

    def trade(one, other):
        moved = pltpu.roll(jnp.where(lower, other, one), 64, 1)
        return jnp.where(lower, one, moved), jnp.where(lower, moved, other)

    def ordered(strip):
        return jnp.concatenate(
            [strips[strip, pl.ds(side, n // 2, stride=2), :] for side in range(2)], axis=0
        )

    def tables_xt():
        for strip in range(n // 128):
            at = pl.ds(strip * 128, 128)
            strips[strip] = basis_x[:, at]
            xt_high[at, :], xt_low[at, :] = halves(ordered(strip).T)

    def tables_x():
        for strip in range(n // 128):
            at = pl.ds(strip * 128, 128)
            x_high[:, at], x_low[:, at] = halves(ordered(strip))

    def tables_y():
        y_high[...], y_low[...] = halves(basis_y[...])
        column[...] = jnp.broadcast_to(eigen_x[...], (128, n)).T

    def tables_yt():
        yt_high[...], yt_low[...] = halves(basis_y[...].T)

    def gather(plane, side):
        for pair in range(cols_n // 2):
            left = field_ref[:, 2 * pair, :, plane].reshape(half, 128)
            right = field_ref[:, 2 * pair + 1, :, plane].reshape(half, 128)
            even, odd = trade(left, right)
            at = pl.ds(pair * 128, 128)
            for rows, value in ((pl.ds(0, half), even), (pl.ds(half, half), odd)):
                plane_high[side, rows, at], plane_low[side, rows, at] = halves(value)

    def scatter(plane, field):
        for pair in range(cols_n // 2):
            even = field[:half, pair * 128 : pair * 128 + 128]
            odd = field[half:, pair * 128 : pair * 128 + 128]
            left, right = trade(even, odd)
            out_ref[:, 2 * pair, plane] = left.reshape(rows_n, 16, 128)
            out_ref[:, 2 * pair + 1, plane] = right.reshape(rows_n, 16, 128)

    fields = [None] * count

    def into_x(plane):
        side = plane % 2
        fields[plane] = product3(
            (xt_high[...], xt_low[...]), (plane_high[side], plane_low[side])
        )

    def into_y(plane):
        fields[plane] = product3(halves(fields[plane]), (y_high[...], y_low[...]))

    def out_of_y(plane):
        denom = column[:, :1] + (eigen_y[...] + eigen_z[owned + plane])
        fields[plane] = product3(halves(fields[plane] / denom), (yt_high[...], yt_low[...]))

    def out_of_x(plane):
        fields[plane] = product3((x_high[...], x_low[...]), halves(fields[plane]))

    tables_xt()
    gather(0, 0)
    for first in range(0, count, 2):
        second = first + 1
        into_x(first)
        gather(second, 1)
        if first == 0:
            tables_y()
        else:
            scatter(first - 1, fields[first - 1])
        into_x(second)
        if first == 0:
            tables_yt()
            tables_x()
        for stage in (into_y, out_of_y):
            stage(first)
            stage(second)
        out_of_x(first)
        if second + 1 < count:
            gather(second + 1, 0)
        scatter(first, fields[first])
        out_of_x(second)
    scatter(count - 1, fields[count - 1])


VMEM_SPEC = pl.BlockSpec(memory_space=pltpu.VMEM)
HBM_SPEC = pl.BlockSpec(memory_space=pltpu.HBM)


def in_hbm(value):
    return pltpu.with_memory_space_constraint(value, pltpu.HBM)


def limit(mebibytes):
    return pltpu.CompilerParams(vmem_limit_bytes=mebibytes * MIB)


def local(source, basis_x, basis_y, basis_z, eigen_x, eigen_y, eigen_z):
    rows_n, cols_n = lax.axis_size("row"), lax.axis_size("col")
    devices = rows_n * cols_n
    n = basis_z.shape[0]
    square = (n, n)
    lines = source.shape[0] * source.shape[1]

    sent, both_z = pl.pallas_call(
        forward_z,
        out_shape=[
            jax.ShapeDtypeStruct((devices, 2, 32, 128), F32),
            jax.ShapeDtypeStruct((2 * n, n), BF16),
        ],
        in_specs=[HBM_SPEC] * 2,
        out_specs=[VMEM_SPEC] * 2,
        scratch_shapes=[
            pltpu.VMEM((lines, n), F32),
            pltpu.VMEM(square, F32),
            pltpu.VMEM((2, lines * 2, 128), F32),
            pltpu.SemaphoreType.DMA((lines // 512 + 1,)),
        ],
        compiler_params=limit(20),
        name="forward_z",
    )(in_hbm(source.reshape(lines, n)), in_hbm(basis_z))
    sent = sent.reshape(devices, 64, 128)
    field = lax.all_to_all(sent, AXES, split_axis=0, concat_axis=0, tiled=True)

    shape = (rows_n, cols_n, 4, 16, 128)
    field = pl.pallas_call(
        planes,
        out_shape=jax.ShapeDtypeStruct(shape, F32),
        in_specs=[VMEM_SPEC] * 5 + [pl.BlockSpec(memory_space=pltpu.SMEM)],
        out_specs=VMEM_SPEC,
        scratch_shapes=[pltpu.VMEM((n // 128, n, 128), F32)]
        + [pltpu.VMEM(square, BF16)] * 8
        + [pltpu.VMEM((n, 128), F32)]
        + [pltpu.VMEM((2,) + square, BF16)] * 2,
        compiler_params=limit(24),
        name="planes",
    )(
        field.reshape(rows_n, cols_n, 2, 4, 8, 128), basis_x, basis_y,
        eigen_x.reshape(1, n), eigen_y.reshape(1, n), eigen_z,
    )

    field = field.reshape(devices, 64, 128)
    field = lax.all_to_all(field, AXES, split_axis=0, concat_axis=0, tiled=True)
    out = pl.pallas_call(
        backward_z,
        out_shape=jax.ShapeDtypeStruct((lines, n), F32),
        in_specs=[VMEM_SPEC] * 2,
        out_specs=HBM_SPEC,
        scratch_shapes=[
            pltpu.VMEM((2, lines * 2, 128), F32),
            pltpu.VMEM((lines, n), F32),
            pltpu.SemaphoreType.DMA((lines // 256,)),
        ],
        compiler_params=limit(20),
        name="backward_z",
    )(field.reshape(devices, 4, 16, 128), both_z)
    return out.reshape(source.shape)


def solution(mesh):
    placed = (P("row", "col", None), P(), P(), P(), P(), P(), P())
    return jax.shard_map(
        local, mesh=mesh, in_specs=placed, out_specs=P("row", "col", None), check_vma=False
    )
```
